128 devices in a mesh: pipe: 4 (over y_hi, core), exp: 16 (over x, z), pair: 2 (over y_lo).
Axes of the slice: x: 4, y: 4 (y_hi: 2, y_lo: 2; y = y_hi * 2 + y_lo), z: 4, core: 2. Of those that a mesh axis runs over, the one named last changes fastest.
Arguments:
- hidden_in: bfloat16 [4, 1024, 2048], P(None, ('exp', 'pair')), may hold values from -6 to 6
- routes: int32 [4, 4, 1024, 8], P('pipe', None, ('exp', 'pair')), may hold values from 0 to 63, all different within a row; in each aligned block of 32 rows (0 to 31, 32 to 63, ..., all dimensions but the last counted through in order) at most 6 rows name the same one
- gate_probs: float32 [4, 4, 1024, 8], P('pipe', None, ('exp', 'pair')), may hold values from 0.02 to 1
- norm_gain: float32 [4, 2048], P('pipe'), may hold values from 0.1 to 1.9
- w_gate: bfloat16 [4, 64, 2048, 768], P('pipe', ('exp', 'pair')), may hold values from -0.125 to 0.125
- w_up: bfloat16 [4, 64, 2048, 768], P('pipe', ('exp', 'pair')), may hold values from -0.125 to 0.125
- w_down: bfloat16 [4, 64, 768, 2048], P('pipe', ('exp', 'pair')), may hold values from -0.21875 to 0.21875
Outputs:
- layer_outputs: bfloat16 [4, 4, 1024, 2048], P('pipe', None, ('exp', 'pair'))
The draws below stay inside these ranges and needn't reach their ends.
Inputs may be any that keep to these rules, and one draw needn't show every extreme that they name: `routes`: within each layer and micro-batch, the 32 tokens of one device (aligned blocks) name no expert more than 6 times in all, and each token names 8 different experts.
All inputs are finite; a program needn't handle non-finite values.
Results may differ from the reference program's by a relative error of at most 0.01.
Values may be sent and summed in bfloat16 or wider, within the bound.
No kernel may reach another device: no remote copies, remote signals or barrier semaphores. Data moves between devices by JAX's collectives and lax.ppermute only.
A program may use at most 64 MiB of HBM per device.

```python
import math
import jax
import jax.numpy as jnp
import numpy as np
from jax import lax

D = 2048
FF = 768
TOPK = 8
MB = 4
TOK_DEV = 32
EXPERTS = 64
LAYERS = 4
TOKENS = 1024
CAP = 6


def block_scale(rng, shape, shards, least, largest):
    def one(position, parts):
        steps = jax.random.uniform(jax.random.fold_in(jax.random.fold_in(rng, 6), position), (parts,), jnp.float32, least / len(shards), largest / len(shards))
        return jnp.repeat(jnp.exp(steps), shape[position] // parts).reshape((-1,) + (1,) * (len(shape) - position - 1))

    loudness = one(*shards[0])
    for cut in shards[1:]:
        loudness = loudness * one(*cut)
    return loudness


def routed_block(rng, own, number, rows, number_of, top, bound, skew):
    order = jax.random.permutation(rng, number_of)
    packed, common = shares(number_of, rows * top, bound, skew, True), shares(number_of, rows * top, bound, skew, False)
    places = jnp.arange(number_of)

    def named(sizes, rotation):
        used = int((sizes > 0).sum())
        fixed = max(1, used // 4)
        shifted = fixed + (places - fixed + rotation * (used - fixed)) % max(1, number_of - fixed)
        return jnp.zeros((number_of,), jnp.int32).at[order[jnp.where(places < fixed, places, shifted)]].set(jnp.asarray(sizes, jnp.int32))

    sizes = jnp.where(number % 4 == 0, named(packed, number // 4), named(common, number - number // 4 - 1))
    mixed = jax.random.permutation(jax.random.fold_in(own, 3), number_of)
    donor, taker = mixed[0:number_of // 2 * 2:2], mixed[1:number_of // 2 * 2:2]
    margin = jnp.minimum(sizes[donor] - 1, bound - sizes[taker]) // 2
    margin = jnp.where((donor == order[0]) | (taker == order[0]) | (sizes[taker] == 0), 0, jnp.maximum(margin, 0))
    shifted = jax.random.randint(jax.random.fold_in(own, 4), (number_of // 2,), 0, 1 << 20) % (margin + 1)
    sizes = sizes.at[donor].add(-shifted).at[taker].add(shifted)
    labels = jnp.searchsorted(jnp.cumsum(sizes), jnp.arange(rows * top), side="right").astype(jnp.int32)
    grid = labels.reshape(top, rows).T
    grid = grid[jax.random.permutation(jax.random.fold_in(own, 1), rows)]
    rotation = jax.random.randint(jax.random.fold_in(own, 2), (rows, 1), 0, top)
    return jnp.take_along_axis(grid, (jnp.arange(top)[None, :] + rotation) % top, axis=1)


def shares(number_of, total, most, skew, full):
    loads = [(1 << 20) // math.isqrt(grade ** skew) + 1 for grade in range(1, number_of + 1)]
    largest = most if full else min(most, max(-(-total // number_of), total * loads[0] // sum(loads)))
    least = 1 if total - largest >= number_of - 1 else 0
    counts, surplus = [largest] + [least] * (number_of - 1), total - largest - least * (number_of - 1)
    while surplus > 0:
        candidates = [i for i in range(1, number_of) if counts[i] < largest] or [i for i in range(1, number_of) if counts[i] < most]
        mass, remaining = sum([loads[i] for i in candidates]), surplus
        for i in candidates:
            addition = min(most - counts[i], max(1, remaining * loads[i] // mass), surplus)
            counts[i] = counts[i] + addition
            surplus = surplus - addition
    return np.array(counts)


def normal_values(own_key, dims, width, most, shards=(), held_as=jnp.bfloat16):
    drawn = jax.random.normal(own_key, dims, jnp.float32) * width
    if len(shards) > 0:
        drawn = block_scale(own_key, dims, shards, -0.22, 0.18) * drawn
    return jnp.clip(drawn, min=-most, max=most).astype(held_as)


def setup_inputs(seed: int = 0) -> dict:
    key_of = jax.random.split(jax.random.key(seed), 8)
    hidden_in = normal_values(key_of[0], (MB, TOKENS, D), 1.0, 6.0, ((1, 32),))
    routes_keys = jax.random.split(jax.random.fold_in(key_of[1], 1), LAYERS * MB * TOKENS // TOK_DEV)
    routes_turns = jax.random.permutation(jax.random.fold_in(key_of[1], 3), LAYERS * MB * TOKENS // TOK_DEV)
    routes = jax.vmap(lambda own, number: routed_block(jax.random.fold_in(key_of[1], 2), own, number, TOK_DEV, EXPERTS, TOPK, CAP, 2))(routes_keys, routes_turns).reshape((LAYERS, MB, TOKENS, TOPK))
    gate_probs = jnp.clip(jnp.exp(math.log(1.0) - 3.912023 * jax.random.uniform(key_of[2], (LAYERS, MB, TOKENS, TOPK), jnp.float32) ** block_scale(key_of[2], (LAYERS, MB, TOKENS, TOPK), ((0, 4), (2, 32)), -0.2, 0.2)), 0.02, 1.0)
    norm_gain = jnp.clip(1.0 + 0.18 * jax.random.normal(key_of[3], (LAYERS, D), jnp.float32), 0.1, 1.9)
    w_gate = normal_values(key_of[4], (LAYERS, EXPERTS, D, FF), D ** -0.5, 0.125, ((0, 4), (1, 32)))
    w_up = normal_values(key_of[5], (LAYERS, EXPERTS, D, FF), D ** -0.5, 0.125, ((0, 4), (1, 32)))
    w_down = normal_values(key_of[6], (LAYERS, EXPERTS, FF, D), FF ** -0.5, 0.21875, ((0, 4), (1, 32)))
    return {"hidden_in": hidden_in, "routes": routes, "gate_probs": gate_probs, "norm_gain": norm_gain, "w_gate": w_gate, "w_up": w_up, "w_down": w_down}


EPS = 1e-06

def slots_of(block_routes):
    expert_ids = jnp.arange(EXPERTS, dtype=jnp.int32)
    onehot = (block_routes[:, None] == expert_ids[None, :]).astype(jnp.int32)
    before = jnp.cumsum(onehot, axis=0) - onehot
    return lax.optimization_barrier(jnp.sum(before * onehot, axis=1)).astype(jnp.int32)

def moe_layer(state, chosen, probs, gain, wgate, wupper, wdown):
    floated = state.astype(jnp.float32)
    scale = lax.rsqrt(lax.optimization_barrier(jnp.mean(floated * floated, axis=-1, keepdims=True)) + EPS)
    normed = (floated * scale * gain.astype(jnp.float32)).astype(jnp.bfloat16)
    blocks = TOKENS // TOK_DEV
    flat_routes = chosen.reshape(blocks, TOK_DEV * TOPK).astype(jnp.int32)
    slots = jax.vmap(slots_of)(flat_routes)
    columns = (slots + CAP * jnp.arange(blocks, dtype=jnp.int32)[:, None]).reshape(-1)
    rows_ids = flat_routes.reshape(-1)
    buffer = jnp.zeros((EXPERTS, blocks * CAP, D), jnp.bfloat16)
    buffer = buffer.at[rows_ids, columns].set(jnp.repeat(normed, TOPK, axis=0))

    def one_expert(items):
        inputs, gate_w, up_w, down_w = items
        gate = jnp.dot(inputs, gate_w, preferred_element_type=jnp.float32)
        upward = jnp.dot(inputs, up_w, preferred_element_type=jnp.float32)
        hidden = (jax.nn.silu(gate) * upward).astype(jnp.bfloat16)
        return jnp.dot(hidden, down_w, preferred_element_type=jnp.float32).astype(jnp.bfloat16)
    produced = lax.map(one_expert, (buffer, wgate, wupper, wdown))
    picked = produced[rows_ids, columns].reshape(TOKENS, TOPK, D).astype(jnp.float32)
    probs32 = probs.astype(jnp.float32)
    weights = probs32 / lax.optimization_barrier(jnp.sum(probs32, axis=-1, keepdims=True))
    mixed = jnp.einsum('tk,tkd->td', weights, picked)
    return (floated + mixed).astype(jnp.bfloat16)

def reference(hidden_in, routes, gate_probs, norm_gain, w_gate, w_up, w_down):
    current = hidden_in
    outputs = []
    for layer in range(LAYERS):

        def per_batch(items):
            state, chosen, probs = items
            return moe_layer(state, chosen, probs, norm_gain[layer], w_gate[layer], w_up[layer], w_down[layer])
        current = lax.map(per_batch, (current, routes[layer], gate_probs[layer]))
        outputs.append(current)
    return jnp.stack(outputs, axis=0)
```

```python
import functools

import jax
import jax.numpy as jnp
from jax import lax
from jax.experimental import pallas as pl
from jax.experimental.pallas import tpu as pltpu
from jax.sharding import PartitionSpec as P

EPS = 1e-06
F32 = jnp.float32
BF16 = jnp.bfloat16
GROUP = ("exp", "pair")


def dot(a, b):
    return jnp.dot(a, b, preferred_element_type=F32)


def dot_nt(a, b):
    return lax.dot_general(a, b, (((1,), (1,)), ((), ())), preferred_element_type=F32)


def iota(shape, dim):
    return lax.broadcasted_iota(jnp.int32, shape, dim)


def select_matrix(shape, source):
    return jnp.where(iota(shape, 1) == source(iota(shape, 0)), 1.0, 0.0).astype(BF16)


def naming(chosen, experts, values=None):
    tokens, top = chosen.shape
    ids = iota((tokens, experts), 1)
    total = jnp.zeros((tokens, experts), F32)
    for k in range(top):
        value = 1.0 if values is None else values[:, k : k + 1]
        total = total + jnp.where(chosen[:, k : k + 1] == ids, value, 0.0)
    return total


def rank_of(named):
    tokens = named.shape[0]
    earlier = jnp.where(iota((tokens, tokens), 1) < iota((tokens, tokens), 0), 1.0, 0.0)
    return dot(earlier.astype(BF16), named.astype(BF16))


def dispatch_kernel(where_ref, hidden_ref, received_ref, routes_ref, gain_ref, out_ref, state_ref):
    index = where_ref[0]
    experts = out_ref.shape[0] // 4
    width = hidden_ref.shape[2]
    half = width // 2
    state = jnp.where(where_ref[1] == 0, hidden_ref[index], received_ref[...])
    state_ref[...] = state
    floated = state.astype(F32)
    scale = lax.rsqrt(jnp.mean(floated * floated, axis=-1, keepdims=True) + EPS)
    normed = (floated * scale * gain_ref[...]).astype(BF16)
    named = naming(routes_ref[index], experts)
    rank = rank_of(named)
    spread = select_matrix((4 * experts, experts), lambda i: i >> 2)
    named_rows = dot_nt(spread, named.astype(BF16))
    rank_rows = dot_nt(spread, rank.astype(BF16)).astype(jnp.int32)
    row = iota(rank_rows.shape, 0)
    whole = jnp.where(rank_rows == (row & 3), named_rows, 0.0).astype(BF16)
    rest = jnp.where(rank_rows == 4 + ((row & 3) >> 1), named_rows, 0.0)
    left = jnp.where((row & 1) == 0, rest, 0.0).astype(BF16)
    right = jnp.where((row & 1) == 1, rest, 0.0).astype(BF16)
    out_ref[:, :width] = dot(whole, normed).astype(BF16)
    out_ref[:, width:] = (dot(left, normed[:, :half]) + dot(right, normed[:, half:])).astype(BF16)


def combine_kernel(where_ref, returned_ref, state_ref, routes_ref, probs_ref, updated_ref):
    index = where_ref[0]
    experts = returned_ref.shape[0] // 4
    tokens, width = state_ref.shape
    half = width // 2
    chosen = routes_ref[index]
    probs = probs_ref[index]
    weights = probs / jnp.sum(probs, axis=-1, keepdims=True)
    rank = rank_of(naming(chosen, experts))
    weight = naming(chosen, experts, weights)
    high = weight.astype(BF16)
    low = (weight - high.astype(F32)).astype(BF16)
    spread = select_matrix((4 * experts, experts), lambda i: i >> 2)
    rank_x = dot_nt(rank.astype(BF16), spread).astype(jnp.int32)
    both = jnp.concatenate([dot_nt(high, spread), dot_nt(low, spread)], axis=0)
    rank_x = jnp.concatenate([rank_x, rank_x], axis=0)
    col = iota(rank_x.shape, 1)
    whole = jnp.where(rank_x == (col & 3), both, 0.0).astype(BF16)
    rest = jnp.where(rank_x == 4 + ((col & 3) >> 1), both, 0.0)
    left = jnp.where((col & 1) == 0, rest, 0.0).astype(BF16)
    right = jnp.where((col & 1) == 1, rest, 0.0).astype(BF16)
    first = dot(whole, returned_ref[:, :width])
    tail = dot(jnp.concatenate([left, right], axis=0), returned_ref[:, width:])
    mixed = first[:tokens] + first[tokens:]
    mixed_left = tail[:tokens] + tail[tokens : 2 * tokens]
    mixed_right = tail[2 * tokens : 3 * tokens] + tail[3 * tokens :]
    floated = state_ref[...].astype(F32)
    updated_ref[:, :half] = (floated[:, :half] + mixed[:, :half] + mixed_left).astype(BF16)
    updated_ref[:, half:] = (floated[:, half:] + mixed[:, half:] + mixed_right).astype(BF16)


def expert_kernel(
    arrived_ref, gate_hbm, up_hbm, down_hbm, out_ref, gate_v, up_v, down_v, rows_v, acc_v, made_v, sems, *, cuts
):
    local, width, hidden = gate_v.shape
    groups = arrived_ref.shape[0] // 8
    half = width // 2
    cut = hidden // cuts

    def copies(e, f):
        part = pl.ds(f * cut, cut)
        return (
            pltpu.make_async_copy(gate_hbm.at[e, :, part], gate_v.at[e, :, part], sems.at[0, e, f]),
            pltpu.make_async_copy(up_hbm.at[e, :, part], up_v.at[e, :, part], sems.at[1, e, f]),
            pltpu.make_async_copy(down_hbm.at[e, part, :], down_v.at[e, part, :], sems.at[2, e, f]),
        )

    for e in range(local):
        for f in range(cuts):
            for copy in copies(e, f):
                copy.start()
    for e in range(local):
        pick = select_matrix((4 * groups, 8 * groups), lambda i: 8 * (i >> 2) + 4 * e + (i & 3))
        rows_v[: 4 * groups] = dot(pick, arrived_ref[:, :width]).astype(BF16)
        for q in range(2):
            pick = select_matrix((2 * groups, 8 * groups), lambda i: 8 * (i >> 1) + 4 * e + 2 * (i & 1) + q)
            rows_v[4 * groups :, q * half : (q + 1) * half] = dot(pick, arrived_ref[:, width:]).astype(BF16)
        for f in range(cuts):
            gate_copy, up_copy, down_copy = copies(e, f)
            part = slice(f * cut, (f + 1) * cut)
            gate_copy.wait()
            gate = dot(rows_v[...], gate_v[e, :, part])
            up_copy.wait()
            upward = dot(rows_v[...], up_v[e, :, part])
            mid = (jax.nn.silu(gate) * upward).astype(BF16)
            down_copy.wait()
            product = dot(mid, down_v[e, part, :])
            if f == 0:
                acc_v[...] = product
            elif f < cuts - 1:
                acc_v[...] += product
            else:
                made_v[e] = (acc_v[...] + product).astype(BF16)
    out = jnp.zeros((8 * groups, width), F32)
    tail = jnp.zeros((8 * groups, half), F32)
    for e in range(local):
        target = iota((8 * groups, 4 * groups), 0)
        place = jnp.where(
            (iota(target.shape, 1) == 4 * (target >> 3) + (target & 3)) & (((target >> 2) & 1) == e), 1.0, 0.0
        ).astype(BF16)
        out = out + dot(place, made_v[e, : 4 * groups])
        for q in range(2):
            target = iota((8 * groups, 2 * groups), 0)
            place = jnp.where(
                (iota(target.shape, 1) == 2 * (target >> 3) + ((target >> 1) & 1))
                & (((target >> 2) & 1) == e)
                & ((target & 1) == q),
                1.0,
                0.0,
            ).astype(BF16)
            tail = tail + dot(place, made_v[e, 4 * groups :, q * half : (q + 1) * half])
    out_ref[:, :width] = out.astype(BF16)
    out_ref[:, width:] = tail.astype(BF16)


def on_device(hidden_in, routes, gate_probs, norm_gain, w_gate, w_up, w_down):
    section = lax.axis_index("pipe")
    stages = lax.axis_size("pipe")
    micro, tokens, width = hidden_in.shape
    groups = lax.axis_size(GROUP)
    local, hidden = w_gate.shape[1], w_gate.shape[3]
    assert local == 2 and routes.shape[3] * tokens == 4 * local * groups
    rows = 8 * groups
    wide = width + width // 2
    smem = pl.BlockSpec(memory_space=pltpu.SMEM)
    vmem = pl.BlockSpec(memory_space=pltpu.VMEM)
    hbm = pl.BlockSpec(memory_space=pl.ANY)
    packet = jax.ShapeDtypeStruct((rows, wide), BF16)
    token_rows = jax.ShapeDtypeStruct((tokens, width), BF16)
    cuts = 3

    dispatch = pl.pallas_call(
        dispatch_kernel,
        out_shape=(packet, token_rows),
        in_specs=[smem, vmem, vmem, vmem, vmem],
        out_specs=(vmem, vmem),
        name="dispatch",
    )
    experts = pl.pallas_call(
        functools.partial(expert_kernel, cuts=cuts),
        out_shape=packet,
        in_specs=[vmem, hbm, hbm, hbm],
        out_specs=vmem,
        scratch_shapes=[
            pltpu.VMEM((local, width, hidden), BF16),
            pltpu.VMEM((local, width, hidden), BF16),
            pltpu.VMEM((local, hidden, width), BF16),
            pltpu.VMEM((6 * groups, width), BF16),
            pltpu.VMEM((6 * groups, width), F32),
            pltpu.VMEM((local, 6 * groups, width), BF16),
            pltpu.SemaphoreType.DMA((3, local, cuts)),
        ],
        compiler_params=pltpu.CompilerParams(vmem_limit_bytes=44 * 2**20),
        name="experts",
    )
    combine = pl.pallas_call(
        combine_kernel,
        out_shape=token_rows,
        in_specs=[smem, vmem, vmem, vmem, vmem],
        out_specs=vmem,
        name="combine",
    )

    def exchange(packets):
        return lax.all_to_all(packets, GROUP, split_axis=0, concat_axis=0, tiled=True)

    def advance(step, carry):
        received, made = carry
        index = jnp.clip(step - section, 0, micro - 1)
        where = jnp.stack([index, section]).astype(jnp.int32)
        packets, state = dispatch(where, hidden_in, received, routes[0], norm_gain)
        arrived = exchange(packets)
        produced = experts(arrived, w_gate[0], w_up[0], w_down[0])
        returned = exchange(produced)
        updated = combine(where, returned, state, routes[0], gate_probs[0])
        made = lax.dynamic_update_index_in_dim(made, updated, step, 0)
        received = lax.ppermute(updated, "pipe", [(s, s + 1) for s in range(stages - 1)])
        return received, made

    steps = micro + stages - 1
    start = (jnp.zeros((tokens, width), BF16), jnp.zeros((steps, tokens, width), BF16))
    received, made = lax.fori_loop(0, steps, advance, start)
    saved = lax.dynamic_slice_in_dim(made, section, micro, 0)
    return saved[None]


def solution(mesh):
    in_specs = (
        P(None, GROUP, None),
        P("pipe", None, GROUP, None),
        P("pipe", None, GROUP, None),
        P("pipe", None),
        P("pipe", GROUP, None, None),
        P("pipe", GROUP, None, None),
        P("pipe", GROUP, None, None),
    )
    out_specs = P("pipe", None, GROUP, None)
    return jax.shard_map(on_device, mesh=mesh, in_specs=in_specs, out_specs=out_specs, check_vma=False)
```

```python
import functools

import jax
import jax.numpy as jnp
from jax import lax
from jax.experimental import pallas as pl
from jax.experimental.pallas import tpu as pltpu
from jax.sharding import PartitionSpec as P

EPS = 1e-06
F32 = jnp.float32
BF16 = jnp.bfloat16
GROUP = ("exp", "pair")


def dot(a, b):
    return jnp.dot(a, b, preferred_element_type=F32)


def dot_nt(a, b):
    return lax.dot_general(a, b, (((1,), (1,)), ((), ())), preferred_element_type=F32)


def iota(shape, dim):
    return lax.broadcasted_iota(jnp.int32, shape, dim)


def select_matrix(shape, source):
    return jnp.where(iota(shape, 1) == source(iota(shape, 0)), 1.0, 0.0).astype(BF16)


def naming(chosen, experts, values=None):
    tokens, top = chosen.shape
    ids = iota((tokens, experts), 1)
    total = jnp.zeros((tokens, experts), F32)
    for k in range(top):
        value = 1.0 if values is None else values[:, k : k + 1]
        total = total + jnp.where(chosen[:, k : k + 1] == ids, value, 0.0)
    return total


def rank_of(named, block):
    tokens = named.shape[0]
    row, col = iota((tokens, tokens), 0), iota((tokens, tokens), 1)
    earlier = jnp.where((col < row) & (col // block == row // block), 1.0, 0.0)
    return dot(earlier.astype(BF16), named.astype(BF16))


def whole_slots(i):
    return (i >> 3) & 1, (i >> 2) & 1, i & 3


def half_slots(i):
    return (i >> 2) & 1, (i >> 1) & 1, 4 + (i & 1)


def spread_of(rows, experts, side, slots):
    return select_matrix((rows, experts), lambda i: 4 * (i >> 4) + 2 * side + slots(i)[0])


def dispatch_kernel(
    where_ref, hidden_ref, other_ref, same_ref, cross_ref, routes_ref, routes_other_ref, gain_ref, out_ref, state_ref, *, experts
):
    index, section, side = where_ref[0], where_ref[1], where_ref[2]
    rows = out_ref.shape[0]
    tokens = hidden_ref.shape[1]
    width = state_ref.shape[1]
    half = width // 2
    same, cross = same_ref[...].astype(F32), cross_ref[...].astype(F32)
    mine = jnp.where(section == 0, hidden_ref[index], (same[:tokens] + cross[tokens:]).astype(BF16))
    others = jnp.where(section == 0, other_ref[index], (same[tokens:] + cross[:tokens]).astype(BF16))
    state = jnp.concatenate([mine, others], axis=0)
    state_ref[...] = state
    floated = state.astype(F32)
    scale = lax.rsqrt(jnp.mean(floated * floated, axis=-1, keepdims=True) + EPS)
    normed = (floated * scale * gain_ref[...]).astype(BF16)
    named = naming(jnp.concatenate([routes_ref[index], routes_other_ref[index]], axis=0), experts)
    rank = rank_of(named, tokens).astype(BF16)
    named = named.astype(BF16)

    def pick(slots):
        spread = spread_of(rows, experts, side, slots)
        named_rows = dot_nt(spread, named)
        rank_rows = dot_nt(spread, rank).astype(jnp.int32)
        row, col = iota(rank_rows.shape, 0), iota(rank_rows.shape, 1)
        _, block, slot = slots(row)
        return jnp.where((col // tokens == block) & (rank_rows == slot), named_rows, 0.0), row

    whole, _ = pick(whole_slots)
    out_ref[:, :width] = dot(whole.astype(BF16), normed).astype(BF16)
    rest, row = pick(half_slots)
    first = ((row >> 3) & 1) == 0
    left = jnp.where(first, rest, 0.0).astype(BF16)
    right = jnp.where(first, 0.0, rest).astype(BF16)
    out_ref[:, width:] = (dot(left, normed[:, :half]) + dot(right, normed[:, half:])).astype(BF16)


def combine_kernel(
    where_ref, returned_ref, state_ref, routes_ref, routes_other_ref, probs_ref, probs_other_ref, part_ref, *, experts
):
    index, side = where_ref[0], where_ref[2]
    rows = returned_ref.shape[0]
    both, width = state_ref.shape
    tokens = both // 2
    half = width // 2
    chosen = jnp.concatenate([routes_ref[index], routes_other_ref[index]], axis=0)
    probs = jnp.concatenate([probs_ref[index], probs_other_ref[index]], axis=0)
    weights = probs / jnp.sum(probs, axis=-1, keepdims=True)
    rank = rank_of(naming(chosen, experts), tokens).astype(BF16)
    weight = naming(chosen, experts, weights)
    high = weight.astype(BF16)
    low = (weight - high.astype(F32)).astype(BF16)

    def pick(slots):
        spread = spread_of(rows, experts, side, slots)
        rank_x = dot_nt(rank, spread).astype(jnp.int32)
        row, col = iota(rank_x.shape, 0), iota(rank_x.shape, 1)
        _, block, slot = slots(col)
        held = (row // tokens == block) & (rank_x == slot)
        return [jnp.where(held, dot_nt(part, spread), 0.0) for part in (high, low)], col

    whole, _ = pick(whole_slots)
    sums = dot(jnp.concatenate(whole, axis=0).astype(BF16), returned_ref[:, :width])
    rest, col = pick(half_slots)
    first = ((col >> 3) & 1) == 0
    halves = [jnp.where(first, part, 0.0) for part in rest] + [jnp.where(first, 0.0, part) for part in rest]
    tail = dot(jnp.concatenate(halves, axis=0).astype(BF16), returned_ref[:, width:])
    mixed = sums[:both] + sums[both:]
    mixed_left = tail[:both] + tail[both : 2 * both]
    mixed_right = tail[2 * both : 3 * both] + tail[3 * both :]
    shared = state_ref[...].astype(F32) * 0.5
    part_ref[:, :half] = (shared[:, :half] + mixed[:, :half] + mixed_left).astype(BF16)
    part_ref[:, half:] = (shared[:, half:] + mixed[:, half:] + mixed_right).astype(BF16)


def expert_kernel(
    arrived_ref, gate_hbm, up_hbm, down_hbm, out_ref, gate_v, up_v, down_v, rows_v, rest_v, mid_v, made_v, sems, *, cuts
):
    local, width, hidden = gate_v.shape
    sources = arrived_ref.shape[0] // 16
    half = width // 2
    cut = hidden // cuts
    full = 8 * sources

    def copies(e, f):
        part = pl.ds(f * cut, cut)
        return (
            pltpu.make_async_copy(gate_hbm.at[e, :, part], gate_v.at[e, :, part], sems.at[0, e, f]),
            pltpu.make_async_copy(up_hbm.at[e, :, part], up_v.at[e, :, part], sems.at[1, e, f]),
        )

    def down_copy(e, f):
        part = pl.ds(f * cut, cut)
        return pltpu.make_async_copy(down_hbm.at[e, part, :], down_v.at[e, part, :], sems.at[2, e, f])

    for e in range(local):
        for f in range(cuts):
            for copy in copies(e, f):
                copy.start()
        for f in range(cuts):
            down_copy(e, f).start()
    for g in range(sources):
        for e in range(local):
            rows_v[e, 8 * g : 8 * g + 8] = arrived_ref[16 * g + 8 * e : 16 * g + 8 * e + 8, :width]
        for q in range(2):
            rest_v[8 * g : 8 * g + 8, q * half : (q + 1) * half] = arrived_ref[16 * g + 8 * q : 16 * g + 8 * q + 8, width:]
    for e in range(local):
        pick = select_matrix((4 * sources, full), lambda i: 8 * (i >> 2) + 4 * e + (i & 3))
        rows_v[e, full:] = dot(pick, rest_v[...]).astype(BF16)
    for e in range(local):
        for f in range(cuts):
            gate_copy, up_copy = copies(e, f)
            part = slice(f * cut, (f + 1) * cut)
            gate_copy.wait()
            gate = dot(rows_v[e], gate_v[e, :, part])
            up_copy.wait()
            upward = dot(rows_v[e], up_v[e, :, part])
            mid_v[:, part] = (jax.nn.silu(gate) * upward).astype(BF16)
        for f in range(cuts):
            down_copy(e, f).wait()
        product = dot(mid_v[...], down_v[e]).astype(BF16)
        made_v[e] = product[full:]
        for g in range(sources):
            out_ref[16 * g + 8 * e : 16 * g + 8 * e + 8, :width] = product[8 * g : 8 * g + 8]
    shape = (full, full)
    target, column = iota(shape, 0), iota(shape, 1)
    source = ((target >> 2) & 1) * (4 * sources) + 4 * (target >> 3) + (target & 3)
    place = jnp.where(column == source, 1.0, 0.0).astype(BF16)
    rest = dot(place, made_v[...].reshape(full, width)).astype(BF16)
    for g in range(sources):
        for q in range(2):
            out_ref[16 * g + 8 * q : 16 * g + 8 * q + 8, width:] = rest[8 * g : 8 * g + 8, q * half : (q + 1) * half]


def on_device(hidden_in, routes, gate_probs, norm_gain, w_gate, w_up, w_down):
    section = lax.axis_index("pipe")
    side = lax.axis_index("pair")
    stages = lax.axis_size("pipe")
    micro, tokens, width = hidden_in.shape
    groups = lax.axis_size(("exp", "pair"))
    local, hidden = w_gate.shape[1], w_gate.shape[3]
    top = routes.shape[3]
    assert local == 2 and lax.axis_size("pair") == 2 and top * tokens == 4 * local * groups
    smem = pl.BlockSpec(memory_space=pltpu.SMEM)
    vmem = pl.BlockSpec(memory_space=pltpu.VMEM)
    hbm = pl.BlockSpec(memory_space=pl.ANY)
    packet = jax.ShapeDtypeStruct((8 * groups, width + width // 2), BF16)
    token_rows = jax.ShapeDtypeStruct((2 * tokens, width), BF16)
    cuts = 3

    dispatch = pl.pallas_call(
        functools.partial(dispatch_kernel, experts=local * groups),
        out_shape=(packet, token_rows),
        in_specs=[smem] + [vmem] * 7,
        out_specs=(vmem, vmem),
        compiler_params=pltpu.CompilerParams(vmem_limit_bytes=16 * 2**20),
        name="dispatch",
    )
    experts = pl.pallas_call(
        functools.partial(expert_kernel, cuts=cuts),
        out_shape=packet,
        in_specs=[vmem, hbm, hbm, hbm],
        out_specs=vmem,
        scratch_shapes=[
            pltpu.VMEM((local, width, hidden), BF16),
            pltpu.VMEM((local, width, hidden), BF16),
            pltpu.VMEM((local, hidden, width), BF16),
            pltpu.VMEM((local, 6 * groups, width), BF16),
            pltpu.VMEM((4 * groups, width), BF16),
            pltpu.VMEM((6 * groups, hidden), BF16),
            pltpu.VMEM((local, 2 * groups, width), BF16),
            pltpu.SemaphoreType.DMA((3, local, cuts)),
        ],
        compiler_params=pltpu.CompilerParams(vmem_limit_bytes=32 * 2**20),
        name="experts",
    )
    combine = pl.pallas_call(
        functools.partial(combine_kernel, experts=local * groups),
        out_shape=token_rows,
        in_specs=[smem] + [vmem] * 6,
        out_specs=vmem,
        compiler_params=pltpu.CompilerParams(vmem_limit_bytes=16 * 2**20),
        name="combine",
    )

    def exchange(packets):
        return lax.all_to_all(packets, "exp", split_axis=0, concat_axis=0, tiled=True)

    swap = [(0, 1), (1, 0)]
    stage_pair = ("pipe", "pair")
    hidden_other = lax.ppermute(hidden_in, stage_pair, swap)
    routes_other = lax.ppermute(routes[0], "pair", swap)
    probs_other = lax.ppermute(gate_probs[0], "pair", swap)
    onward = [(2 * s + y, 2 * s + 2 + y) for s in range(stages - 1) for y in range(2)]
    across = [(2 * s + y, 2 * s + 3 - y) for s in range(stages - 1) for y in range(2)]

    def advance(step, carry):
        same, cross, made = carry
        index = jnp.clip(step - section, 0, micro - 1)
        where = jnp.stack([index, section, side]).astype(jnp.int32)

        def layer():
            packets, state = dispatch(
                where, hidden_in, hidden_other, same, cross, routes[0], routes_other, norm_gain
            )
            produced = experts(exchange(packets), w_gate[0], w_up[0], w_down[0])
            return combine(
                where, exchange(produced), state, routes[0], routes_other, gate_probs[0], probs_other
            )

        part = lax.cond((step >= section) & (step < section + micro), layer, lambda: same)
        made = lax.dynamic_update_index_in_dim(made, part, step, 0)
        same = lax.ppermute(part, stage_pair, onward)
        cross = lax.ppermute(part, stage_pair, across)
        return same, cross, made

    steps = micro + stages - 1
    blank = jnp.zeros((2 * tokens, width), BF16)
    start = (blank, blank, jnp.zeros((steps, 2 * tokens, width), BF16))
    same, cross, made = lax.fori_loop(0, steps, advance, start)
    own = lax.dynamic_slice(made, (section, 0, 0), (micro, tokens, width))
    given = lax.dynamic_slice(made, (section, tokens, 0), (micro, tokens, width))
    taken = lax.ppermute(given, "pair", swap)
    return (own.astype(F32) + taken.astype(F32)).astype(BF16)[None]


def solution(mesh):
    in_specs = (
        P(None, GROUP, None),
        P("pipe", None, GROUP, None),
        P("pipe", None, GROUP, None),
        P("pipe", None),
        P("pipe", GROUP, None, None),
        P("pipe", GROUP, None, None),
        P("pipe", GROUP, None, None),
    )
    out_specs = P("pipe", None, GROUP, None)
    return jax.shard_map(on_device, mesh=mesh, in_specs=in_specs, out_specs=out_specs, check_vma=False)
```

```python
import functools

import jax
import jax.numpy as jnp
from jax import lax
from jax.experimental import pallas as pl
from jax.experimental.pallas import tpu as pltpu
from jax.sharding import PartitionSpec as P

EPS = 1e-06
STAGGER_NS = 8000
F32 = jnp.float32
BF16 = jnp.bfloat16
GROUP = ("exp", "pair")


def dot(a, b):
    return jnp.dot(a, b, preferred_element_type=F32)


def dot_nt(a, b):
    return lax.dot_general(a, b, (((1,), (1,)), ((), ())), preferred_element_type=F32)


def iota(shape, dim):
    return lax.broadcasted_iota(jnp.int32, shape, dim)


def select_matrix(shape, source):
    return jnp.where(iota(shape, 1) == source(iota(shape, 0)), 1.0, 0.0).astype(BF16)


def naming(chosen, experts, values=None):
    tokens, top = chosen.shape
    ids = iota((tokens, experts), 1)
    total = jnp.zeros((tokens, experts), F32)
    for k in range(top):
        value = 1.0 if values is None else values[:, k : k + 1]
        total = total + jnp.where(chosen[:, k : k + 1] == ids, value, 0.0)
    return total


def rank_of(named, block):
    tokens = named.shape[0]
    row, col = iota((tokens, tokens), 0), iota((tokens, tokens), 1)
    earlier = jnp.where((col < row) & (col // block == row // block), 1.0, 0.0)
    return dot(earlier.astype(BF16), named.astype(BF16))


def whole_slots(i):
    return (i >> 3) & 1, (i >> 2) & 1, i & 3


def half_slots(i):
    return (i >> 2) & 1, (i >> 1) & 1, 4 + (i & 1)


def spread_of(rows, experts, side, slots):
    return select_matrix((rows, experts), lambda i: 4 * (i >> 4) + 2 * side + slots(i)[0])


def dispatch_kernel(
    where_ref, hidden_ref, other_ref, same_ref, cross_ref, routes_ref, routes_other_ref, gain_ref, out_ref, state_ref, *, experts
):
    index, section, side = where_ref[0], where_ref[1], where_ref[2]

    @pl.when(where_ref[3] == 1)
    def _():
        pl.delay(STAGGER_NS)

    rows = out_ref.shape[0]
    tokens = hidden_ref.shape[1]
    width = state_ref.shape[1]
    half = width // 2
    same, cross = same_ref[...].astype(F32), cross_ref[...].astype(F32)
    mine = jnp.where(section == 0, hidden_ref[index], (same[:tokens] + cross[tokens:]).astype(BF16))
    others = jnp.where(section == 0, other_ref[index], (same[tokens:] + cross[:tokens]).astype(BF16))
    state = jnp.concatenate([mine, others], axis=0)
    state_ref[...] = state
    floated = state.astype(F32)
    scale = lax.rsqrt(jnp.mean(floated * floated, axis=-1, keepdims=True) + EPS)
    normed = (floated * scale * gain_ref[...]).astype(BF16)
    named = naming(jnp.concatenate([routes_ref[index], routes_other_ref[index]], axis=0), experts)
    rank = rank_of(named, tokens).astype(BF16)
    named = named.astype(BF16)

    def pick(slots):
        spread = spread_of(rows, experts, side, slots)
        named_rows = dot_nt(spread, named)
        rank_rows = dot_nt(spread, rank).astype(jnp.int32)
        row, col = iota(rank_rows.shape, 0), iota(rank_rows.shape, 1)
        _, block, slot = slots(row)
        return jnp.where((col // tokens == block) & (rank_rows == slot), named_rows, 0.0), row

    whole, _ = pick(whole_slots)
    out_ref[:, :width] = dot(whole.astype(BF16), normed).astype(BF16)
    rest, row = pick(half_slots)
    first = ((row >> 3) & 1) == 0
    left = jnp.where(first, rest, 0.0).astype(BF16)
    right = jnp.where(first, 0.0, rest).astype(BF16)
    out_ref[:, width:] = (dot(left, normed[:, :half]) + dot(right, normed[:, half:])).astype(BF16)


def combine_kernel(
    where_ref, returned_ref, state_ref, routes_ref, routes_other_ref, probs_ref, probs_other_ref, part_ref, *, experts
):
    index, side = where_ref[0], where_ref[2]
    rows = returned_ref.shape[0]
    both, width = state_ref.shape
    tokens = both // 2
    half = width // 2
    chosen = jnp.concatenate([routes_ref[index], routes_other_ref[index]], axis=0)
    probs = jnp.concatenate([probs_ref[index], probs_other_ref[index]], axis=0)
    weights = probs / jnp.sum(probs, axis=-1, keepdims=True)
    rank = rank_of(naming(chosen, experts), tokens).astype(BF16)
    weight = naming(chosen, experts, weights)
    high = weight.astype(BF16)
    low = (weight - high.astype(F32)).astype(BF16)

    def pick(slots):
        spread = spread_of(rows, experts, side, slots)
        rank_x = dot_nt(rank, spread).astype(jnp.int32)
        row, col = iota(rank_x.shape, 0), iota(rank_x.shape, 1)
        _, block, slot = slots(col)
        held = (row // tokens == block) & (rank_x == slot)
        return [jnp.where(held, dot_nt(part, spread), 0.0) for part in (high, low)], col

    whole, _ = pick(whole_slots)
    sums = dot(jnp.concatenate(whole, axis=0).astype(BF16), returned_ref[:, :width])
    rest, col = pick(half_slots)
    first = ((col >> 3) & 1) == 0
    halves = [jnp.where(first, part, 0.0) for part in rest] + [jnp.where(first, 0.0, part) for part in rest]
    tail = dot(jnp.concatenate(halves, axis=0).astype(BF16), returned_ref[:, width:])
    mixed = sums[:both] + sums[both:]
    mixed_left = tail[:both] + tail[both : 2 * both]
    mixed_right = tail[2 * both : 3 * both] + tail[3 * both :]
    shared = state_ref[...].astype(F32) * 0.5
    part_ref[:, :half] = (shared[:, :half] + mixed[:, :half] + mixed_left).astype(BF16)
    part_ref[:, half:] = (shared[:, half:] + mixed[:, half:] + mixed_right).astype(BF16)


def expert_kernel(
    arrived_ref, gate_hbm, up_hbm, down_hbm, out_ref, gate_v, up_v, down_v, rows_v, rest_v, mid_v, made_v, sems, *, cuts
):
    local, width, hidden = gate_v.shape
    sources = arrived_ref.shape[0] // 16
    half = width // 2
    cut = hidden // cuts
    full = 8 * sources

    def copies(e, f):
        part = pl.ds(f * cut, cut)
        return (
            pltpu.make_async_copy(gate_hbm.at[e, :, part], gate_v.at[e, :, part], sems.at[0, e, f]),
            pltpu.make_async_copy(up_hbm.at[e, :, part], up_v.at[e, :, part], sems.at[1, e, f]),
        )

    def down_copy(e, f):
        part = pl.ds(f * cut, cut)
        return pltpu.make_async_copy(down_hbm.at[e, part, :], down_v.at[e, part, :], sems.at[2, e, f])

    for e in range(local):
        for f in range(cuts):
            for copy in copies(e, f):
                copy.start()
        for f in range(cuts):
            down_copy(e, f).start()
    for g in range(sources):
        for e in range(local):
            rows_v[e, 8 * g : 8 * g + 8] = arrived_ref[16 * g + 8 * e : 16 * g + 8 * e + 8, :width]
        for q in range(2):
            rest_v[8 * g : 8 * g + 8, q * half : (q + 1) * half] = arrived_ref[16 * g + 8 * q : 16 * g + 8 * q + 8, width:]
    for e in range(local):
        pick = select_matrix((4 * sources, full), lambda i: 8 * (i >> 2) + 4 * e + (i & 3))
        rows_v[e, full:] = dot(pick, rest_v[...]).astype(BF16)
    for e in range(local):
        for f in range(cuts):
            gate_copy, up_copy = copies(e, f)
            part = slice(f * cut, (f + 1) * cut)
            gate_copy.wait()
            gate = dot(rows_v[e], gate_v[e, :, part])
            up_copy.wait()
            upward = dot(rows_v[e], up_v[e, :, part])
            mid_v[:, part] = (jax.nn.silu(gate) * upward).astype(BF16)
        for f in range(cuts):
            down_copy(e, f).wait()
        product = dot(mid_v[...], down_v[e]).astype(BF16)
        made_v[e] = product[full:]
        for g in range(sources):
            out_ref[16 * g + 8 * e : 16 * g + 8 * e + 8, :width] = product[8 * g : 8 * g + 8]
    shape = (full, full)
    target, column = iota(shape, 0), iota(shape, 1)
    source = ((target >> 2) & 1) * (4 * sources) + 4 * (target >> 3) + (target & 3)
    place = jnp.where(column == source, 1.0, 0.0).astype(BF16)
    rest = dot(place, made_v[...].reshape(full, width)).astype(BF16)
    for g in range(sources):
        for q in range(2):
            out_ref[16 * g + 8 * q : 16 * g + 8 * q + 8, width:] = rest[8 * g : 8 * g + 8, q * half : (q + 1) * half]


def on_device(hidden_in, routes, gate_probs, norm_gain, w_gate, w_up, w_down):
    section = lax.axis_index("pipe")
    side = lax.axis_index("pair")
    stages = lax.axis_size("pipe")
    micro, tokens, width = hidden_in.shape
    groups = lax.axis_size(("exp", "pair"))
    local, hidden = w_gate.shape[1], w_gate.shape[3]
    top = routes.shape[3]
    assert local == 2 and lax.axis_size("pair") == 2 and top * tokens == 4 * local * groups
    smem = pl.BlockSpec(memory_space=pltpu.SMEM)
    vmem = pl.BlockSpec(memory_space=pltpu.VMEM)
    hbm = pl.BlockSpec(memory_space=pl.ANY)
    packet = jax.ShapeDtypeStruct((8 * groups, width + width // 2), BF16)
    token_rows = jax.ShapeDtypeStruct((2 * tokens, width), BF16)
    cuts = 3

    dispatch = pl.pallas_call(
        functools.partial(dispatch_kernel, experts=local * groups),
        out_shape=(packet, token_rows),
        in_specs=[smem] + [vmem] * 7,
        out_specs=(vmem, vmem),
        compiler_params=pltpu.CompilerParams(vmem_limit_bytes=16 * 2**20),
        name="dispatch",
    )
    experts = pl.pallas_call(
        functools.partial(expert_kernel, cuts=cuts),
        out_shape=packet,
        in_specs=[vmem, hbm, hbm, hbm],
        out_specs=vmem,
        scratch_shapes=[
            pltpu.VMEM((local, width, hidden), BF16),
            pltpu.VMEM((local, width, hidden), BF16),
            pltpu.VMEM((local, hidden, width), BF16),
            pltpu.VMEM((local, 6 * groups, width), BF16),
            pltpu.VMEM((4 * groups, width), BF16),
            pltpu.VMEM((6 * groups, hidden), BF16),
            pltpu.VMEM((local, 2 * groups, width), BF16),
            pltpu.SemaphoreType.DMA((3, local, cuts)),
        ],
        compiler_params=pltpu.CompilerParams(vmem_limit_bytes=32 * 2**20),
        name="experts",
    )
    combine = pl.pallas_call(
        functools.partial(combine_kernel, experts=local * groups),
        out_shape=token_rows,
        in_specs=[smem] + [vmem] * 6,
        out_specs=vmem,
        compiler_params=pltpu.CompilerParams(vmem_limit_bytes=16 * 2**20),
        name="combine",
    )

    def exchange(packets):
        return lax.all_to_all(packets, "exp", split_axis=0, concat_axis=0, tiled=True)

    swap = [(0, 1), (1, 0)]
    stage_pair = ("pipe", "pair")
    hidden_other = lax.ppermute(hidden_in, stage_pair, swap)
    routes_other = lax.ppermute(routes[0], "pair", swap)
    probs_other = lax.ppermute(gate_probs[0], "pair", swap)
    onward = [(2 * s + y, 2 * s + 2 + y) for s in range(stages - 1) for y in range(2)]
    across = [(2 * s + y, 2 * s + 3 - y) for s in range(stages - 1) for y in range(2)]

    steps = micro + stages - 1

    def advance(step, carry):
        same, cross, made = carry
        index = jnp.clip(step - section, 0, micro - 1)
        late = (section == 1) & (index < micro - 1)
        where = jnp.stack([index, section, side, late.astype(jnp.int32)])

        def layer():
            packets, state = dispatch(
                where, hidden_in, hidden_other, same, cross, routes[0], routes_other, norm_gain
            )
            produced = experts(exchange(packets), w_gate[0], w_up[0], w_down[0])
            return combine(
                where, exchange(produced), state, routes[0], routes_other, gate_probs[0], probs_other
            )

        part = lax.cond((step >= section) & (step < section + micro), layer, lambda: same)
        made = lax.dynamic_update_index_in_dim(made, part, step, 0)

        def relay():
            return lax.ppermute(part, stage_pair, onward), lax.ppermute(part, stage_pair, across)

        same, cross = lax.cond(step < steps - 1, relay, lambda: (same, cross))
        return same, cross, made

    blank = jnp.zeros((2 * tokens, width), BF16)
    start = (blank, blank, jnp.zeros((steps, 2 * tokens, width), BF16))
    same, cross, made = lax.fori_loop(0, steps, advance, start)
    own = lax.dynamic_slice(made, (section, 0, 0), (micro, tokens, width))
    given = lax.dynamic_slice(made, (section, tokens, 0), (micro, tokens, width))
    taken = lax.ppermute(given, "pair", swap)
    return (own.astype(F32) + taken.astype(F32)).astype(BF16)[None]


def solution(mesh):
    in_specs = (
        P(None, GROUP, None),
        P("pipe", None, GROUP, None),
        P("pipe", None, GROUP, None),
        P("pipe", None),
        P("pipe", GROUP, None, None),
        P("pipe", GROUP, None, None),
        P("pipe", GROUP, None, None),
    )
    out_specs = P("pipe", None, GROUP, None)
    return jax.shard_map(on_device, mesh=mesh, in_specs=in_specs, out_specs=out_specs, check_vma=False)
```
